768 devices in a mesh: shard: 64 (over x, y, core), rep: 12 (over z).
Axes of the slice: x: 4, y: 8, z: 12, core: 2. Of those that a mesh axis runs over, the one named last changes fastest.
Arguments:
- grad_parts: bfloat16 [12, 512, 196608], P('rep', 'shard'), may hold values from -12 to 12
- owner_plan: int32 [12, 32], P('rep'), may hold values from 0 to 63, as said below
- refresh: int32 [12, 16], P('rep'), may hold values from 0 to 63, as said below
- roots: bfloat16 [12, 64, 2, 512, 512], P('rep', 'shard'), may hold values from -0.02 to 0.52
Outputs:
- update: bfloat16 [512, 196608], P('shard', 'rep')
The draws below stay inside these ranges and needn't reach their ends.
Inputs may be any that keep to these rules, and one draw needn't show every extreme that they name: `owner_plan`: within each replica's row the 32 owners are distinct; otherwise the assignment is arbitrary. `refresh`: entry 2 b + s names side s (0 left, 1 right) of block b of the row's replica; no block appears twice in a row.
All inputs are finite; a program needn't handle non-finite values.
Results may differ from the reference program's by a relative error of at most 0.018.
Values may be sent and summed in bfloat16 or wider, within the bound.
No kernel may reach another device: no remote copies, remote signals or barrier semaphores. Data moves between devices by JAX's collectives and lax.ppermute only.
A program may use at most 32 MiB of HBM per device.

```python
import math
import jax
import jax.numpy as jnp
from jax import lax

BS = 512
NEWTON = 2
BPR = 32
REFRESH = 16
COLS = 196608
N_SHARD = 64
N_REP = 12


def draw_grad_parts(key, part):
    key_list = jax.random.split(jax.random.fold_in(key, 11), 3)
    log_low = math.log(0.3)
    log_high = math.log(3.0)
    row_scale = jnp.exp(jax.random.uniform(key_list[1], (1, BS, 1), jnp.float32, log_low, log_high))
    col_scale = jnp.exp(jax.random.uniform(key_list[2], (1, 1, COLS), jnp.float32, log_low, log_high))
    values = jnp.clip(jax.random.normal(key_list[0], (N_REP, BS, COLS), jnp.float32), -4.0, 4.0)
    scaled = values * row_scale * col_scale * N_REP ** (-0.5)
    return jnp.clip(scaled, -12.0, 12.0).astype(jnp.bfloat16)


def draw_roots(key, part):
    key_list = jax.random.split(jax.random.fold_in(key, 23), 2)
    full_shape = (N_REP, N_SHARD, 2, BS, BS)
    diagonal = jnp.exp(jax.random.uniform(key_list[0], (N_REP, N_SHARD, 2, BS, 1), jnp.float32, math.log(0.25), math.log(0.5)))
    jitter = 0.004 * jnp.clip(jax.random.normal(key_list[1], full_shape, jnp.float32), -4.0, 4.0)
    identity = (jnp.arange(BS)[:, None] == jnp.arange(BS)[None, :]).astype(jnp.float32)
    return (jitter + diagonal * identity).astype(jnp.bfloat16)


def draw_owner_plan(key, part):
    key_list = jax.random.split(jax.random.fold_in(key, 37), N_REP)

    def owner_row(subkey):
        return jax.random.permutation(subkey, N_SHARD)[:BPR]
    return jax.vmap(owner_row)(key_list).astype(jnp.int32)


def draw_refresh(key, part):
    key_list = jax.random.split(jax.random.fold_in(key, 41), N_REP)

    def refresh_row(subkey):
        key_first, second = jax.random.split(subkey)
        chosen = jax.random.permutation(key_first, BPR)[:REFRESH]
        side_bits = jax.random.randint(second, (REFRESH,), 0, 2)
        return 2 * chosen + side_bits
    return jax.vmap(refresh_row)(key_list).astype(jnp.int32)


def setup_inputs(seed: int = 0) -> dict:
    keys = jax.random.split(jax.random.key(seed), 5)
    return {
        "grad_parts": draw_grad_parts(jax.random.fold_in(keys[4], 71), 0),
        "owner_plan": draw_owner_plan(jax.random.fold_in(keys[4], 71), 0),
        "refresh": draw_refresh(jax.random.fold_in(keys[4], 71), 0),
        "roots": draw_roots(jax.random.fold_in(keys[4], 71), 0),
    }


damping = 0.1

def product(first_mat, second_mat):
    return jnp.dot(first_mat, second_mat, precision=lax.Precision.HIGHEST, preferred_element_type=jnp.float32)

def inverse_root(statistic):
    matrix_size = statistic.shape[0]
    identity = jnp.eye(matrix_size, dtype=jnp.float32)
    damped = statistic + (damping * jnp.trace(statistic) / matrix_size + 1e-06) * identity
    norm_scale = 2.5 / jnp.sqrt(jnp.sum(damped * damped))
    current = identity * jnp.sqrt(jnp.sqrt(norm_scale))
    moment = damped * norm_scale
    for repeat in range(NEWTON):
        factor = (5.0 * identity - moment) * 0.25
        current = product(current, factor)
        square = product(factor, factor)
        moment = product(square, product(square, moment))
    return current.astype(jnp.bfloat16)

def reference(grad_parts, owner_plan, refresh, roots):
    summed = lax.optimization_barrier(jnp.sum(grad_parts.astype(jnp.float32), axis=0))
    full_grad = summed.astype(jnp.bfloat16)
    block_count = N_REP * BPR
    all_blocks = full_grad.reshape(BS, block_count, BS).transpose(1, 0, 2)
    replica_of = jnp.arange(block_count, dtype=jnp.int32) // BPR
    local_of = jnp.arange(block_count, dtype=jnp.int32) % BPR
    owner_of = owner_plan.reshape(-1).astype(jnp.int32)
    chosen = refresh[replica_of]

    def per_block(packed):
        grad_block, replica_id, owner_id, local_id, refresh_row = packed
        stored = roots[replica_id, owner_id]
        left_stat = jnp.dot(grad_block, grad_block.T, preferred_element_type=jnp.float32)
        right_stat = jnp.dot(grad_block.T, grad_block, preferred_element_type=jnp.float32)
        left_new = jnp.any(refresh_row == 2 * local_id)
        right_new = jnp.any(refresh_row == 2 * local_id + 1)
        root_left = lax.cond(left_new, lambda: inverse_root(left_stat), lambda: stored[0])
        root_right = lax.cond(right_new, lambda: inverse_root(right_stat), lambda: stored[1])
        left_part = jnp.dot(root_left, grad_block, preferred_element_type=jnp.float32).astype(jnp.bfloat16)
        precon = jnp.dot(left_part, root_right, preferred_element_type=jnp.float32)
        values = grad_block.astype(jnp.float32)
        graft_scale = jnp.sqrt((jnp.mean(values * values) + 1e-06) / (jnp.mean(precon * precon) + 1e-06))
        return (precon * graft_scale).astype(jnp.bfloat16)
    updates = lax.map(per_block, (all_blocks, replica_of, owner_of, local_of, chosen))
    return updates.transpose(1, 0, 2).reshape(BS, block_count * BS)
```

```python
import functools

import jax
import jax.numpy as jnp
from jax import lax
from jax.experimental import pallas as pl
from jax.experimental.pallas import tpu as pltpu
from jax.sharding import PartitionSpec as P


damping = 0.1

LONG_ARM = {6: 5, 5: 3, 4: 3, 3: 1, 2: 1, 1: 0}
SHORT_ARM = {5: 4, 4: 3, 3: 1, 2: 1, 1: 0}


def steps_before(parent, node):
    children = [c for c in parent if parent[c] == node]
    return 1 + max(steps_before(parent, c) for c in children) if children else 0


def reduce_windows(partial, shards, replicas):
    width = partial.shape[1] // replicas
    here = lax.axis_index("rep")
    toward = jnp.where(lax.axis_index("shard") % 2 == 0, 1, -1)

    def own(window):
        return lax.dynamic_slice(
            partial, (0, ((window + replicas) % replicas) * width), (partial.shape[0], width)
        )

    def pairs(sign, hops):
        out = []
        for shard in range(shards):
            way = sign if shard % 2 == 0 else -sign
            for z in range(replicas):
                out.append((shard * replicas + z, shard * replicas + (z + way * hops) % replicas))
        return out

    arms = []
    for parent, sign in ((LONG_ARM, -1), (SHORT_ARM, 1)):
        arms.append((parent, sign, {node: [] for node in range(7)}))
    last = max(steps_before(parent, node) for parent, _, _ in arms for node in parent)
    for step in range(last + 1):
        todo = []
        for parent, sign, got in arms:
            sends = sorted((n for n in parent if steps_before(parent, n) == step), reverse=True)
            groups = {}
            for place, node in enumerate(sends):
                later = place > 0 and parent[node] != parent[sends[0]]
                groups.setdefault((later, node - parent[node]), []).append(node)
            for (later, hops), nodes in sorted(groups.items()):
                messages = []
                for node in nodes:
                    message = own(here + toward * sign * node)
                    for term in got[node]:
                        message = message + term
                    messages.append(message)
                payload = messages[0] if len(nodes) == 1 else jnp.stack(messages)
                todo.append((later, parent, sign, got, hops, nodes, payload))
        todo.sort(key=lambda entry: entry[0])
        payloads = lax.optimization_barrier(tuple(entry[-1] for entry in todo))
        for (_, parent, sign, got, hops, nodes, _), payload in zip(todo, payloads):
            landed = lax.ppermute(payload, ("shard", "rep"), pairs(sign, hops))
            for place, node in enumerate(nodes):
                got[parent[node]].append(landed if len(nodes) == 1 else landed[place])
    return [own(here)] + [term for _, _, got in arms for term in got[0]]


def dispatch_kernel(terms, owner_ref, *refs):
    term_refs, out_ref = refs[:terms], refs[terms]
    blocks = owner_ref.shape[0]
    width = out_ref.shape[2]
    out_ref[...] = jnp.zeros_like(out_ref)
    for block in range(blocks):
        columns = slice(block * width, (block + 1) * width)
        total = term_refs[0][:, columns].astype(jnp.float32)
        for ref in term_refs[1:]:
            total = total + ref[:, columns].astype(jnp.float32)
        out_ref[owner_ref[block]] = total.astype(jnp.bfloat16)


def mul(first, second):
    return jnp.dot(
        first.astype(jnp.bfloat16), second.astype(jnp.bfloat16), preferred_element_type=jnp.float32
    )


def total_of(values):
    return jnp.sum(jnp.sum(values, axis=0, keepdims=True), axis=1, keepdims=True)


def owner_kernel(me_ref, owner_ref, refresh_ref, grad_ref, roots_ref, out_ref, stat_ref, root_ref):
    size = grad_ref.shape[0]
    me = me_ref[0]
    local_id = jnp.int32(-1)
    for block in range(owner_ref.shape[0]):
        local_id = jnp.where(owner_ref[block] == me, jnp.int32(block), local_id)
    side = jnp.int32(-1)
    for entry in range(refresh_ref.shape[0]):
        value = refresh_ref[entry]
        side = jnp.where(value == 2 * local_id, jnp.int32(0), side)
        side = jnp.where(value == 2 * local_id + 1, jnp.int32(1), side)

    @pl.when(local_id >= 0)
    def _():
        grad = grad_ref[...]
        values = grad.astype(jnp.float32)
        grad_squares = total_of(values * values)

        @pl.when(side != 0)
        def _():
            root_ref[0] = roots_ref[0]

        @pl.when(side != 1)
        def _():
            root_ref[1] = roots_ref[1]

        @pl.when(side == 0)
        def _():
            stat_ref[...] = lax.dot_general(
                grad, grad, (((1,), (1,)), ((), ())), preferred_element_type=jnp.float32
            )

        @pl.when(side == 1)
        def _():
            stat_ref[...] = lax.dot_general(
                grad, grad, (((0,), (0,)), ((), ())), preferred_element_type=jnp.float32
            )

        @pl.when(side >= 0)
        def _():
            rows = lax.broadcasted_iota(jnp.int32, (size, size), 0)
            cols = lax.broadcasted_iota(jnp.int32, (size, size), 1)
            eye = jnp.where(rows == cols, 1.0, 0.0).astype(jnp.float32)
            damped = stat_ref[...] + (damping * grad_squares / size + 1e-06) * eye
            scale = 2.5 / jnp.sqrt(total_of(damped * damped))
            one = damped * scale
            one_low = one.astype(jnp.bfloat16)
            two = mul(one_low, one_low)
            three = mul(two, one_low)
            applied = 1.5625 * one - 0.625 * two + 0.0625 * three
            moment = 1.5625 * applied + mul(0.0625 * two - 0.625 * one, applied)
            root = 1.5625 * eye - 0.3125 * (one + moment) + 0.0625 * mul(one_low, moment)
            root = root * jnp.sqrt(jnp.sqrt(scale))
            root_ref[side] = root.astype(jnp.bfloat16)

        left = jnp.dot(root_ref[0], grad, preferred_element_type=jnp.float32).astype(jnp.bfloat16)
        precon = jnp.dot(left, root_ref[1], preferred_element_type=jnp.float32)
        count = float(size * size)
        graft = jnp.sqrt(
            (grad_squares / count + 1e-06) / (total_of(precon * precon) / count + 1e-06)
        )
        out_ref[...] = (precon * graft).astype(jnp.bfloat16)

    @pl.when(local_id < 0)
    def _():
        out_ref[...] = jnp.zeros_like(out_ref)


def placing_kernel(owner_ref, returned_ref, out_ref):
    width = returned_ref.shape[2]
    for block in range(owner_ref.shape[0]):
        out_ref[:, block * width : (block + 1) * width] = returned_ref[owner_ref[block]]


SMEM = pl.BlockSpec(memory_space=pltpu.SMEM)
VMEM = pl.BlockSpec(memory_space=pltpu.VMEM)


def call(kernel, out_shape, in_specs, scratch, megabytes, name):
    return pl.pallas_call(
        kernel,
        out_shape=jax.ShapeDtypeStruct(out_shape, jnp.bfloat16),
        in_specs=in_specs,
        out_specs=VMEM,
        scratch_shapes=scratch,
        compiler_params=pltpu.CompilerParams(vmem_limit_bytes=megabytes << 20),
        name=name,
    )


def local(shards, replicas, grad_parts, owner_plan, refresh, roots):
    size = roots.shape[-1]
    rows = grad_parts.shape[1]
    owner_row = owner_plan[0]
    blocks = owner_row.shape[0]
    terms = reduce_windows(grad_parts[0], shards, replicas)
    outgoing = call(
        functools.partial(dispatch_kernel, len(terms)),
        (shards, rows, size),
        [SMEM] + [VMEM] * len(terms),
        [],
        8,
        "dispatch",
    )(owner_row, *terms)
    incoming = lax.all_to_all(outgoing, "shard", split_axis=0, concat_axis=0, tiled=True)
    update = call(
        owner_kernel,
        (size, size),
        [SMEM, SMEM, SMEM, VMEM, VMEM],
        [pltpu.VMEM((size, size), jnp.float32), pltpu.VMEM((2, size, size), jnp.bfloat16)],
        32,
        "owner",
    )(
        lax.axis_index("shard").astype(jnp.int32)[None],
        owner_row,
        refresh[0],
        incoming.reshape(size, size),
        roots[0, 0],
    )
    returned = lax.all_to_all(
        update.reshape(shards, rows, size), "shard", split_axis=0, concat_axis=0, tiled=True
    )
    return call(placing_kernel, (rows, blocks * size), [SMEM, VMEM], [], 8, "placing")(
        owner_row, returned
    )


def solution(mesh):
    placed = (
        P("rep", "shard", None),
        P("rep", None),
        P("rep", None),
        P("rep", "shard", None, None, None),
    )
    body = functools.partial(local, mesh.shape["shard"], mesh.shape["rep"])
    return jax.shard_map(
        body, mesh=mesh, in_specs=placed, out_specs=P("shard", "rep"), check_vma=False
    )
```

```python
import functools

import jax
import jax.numpy as jnp
from jax import lax
from jax.experimental import pallas as pl
from jax.experimental.pallas import tpu as pltpu
from jax.sharding import PartitionSpec as P


damping = 0.1

LONG_ARM = {6: 4, 5: 4, 4: 2, 3: 2, 2: 0, 1: 0}
SHORT_ARM = {5: 4, 4: 2, 3: 2, 2: 0, 1: 0}


def steps_before(parent, node):
    children = [c for c in parent if parent[c] == node]
    return 1 + max(steps_before(parent, c) for c in children) if children else 0


def reduce_windows(partial, shards, replicas):
    rows = partial.shape[0]
    width = partial.shape[1] // replicas
    here = lax.axis_index("rep")
    toward = jnp.where(lax.axis_index("shard") % 2 == 0, 1, -1)
    arms = [
        (LONG_ARM, -1, {node: [] for node in range(7)}),
        (SHORT_ARM, 1, {node: [] for node in range(7)}),
    ]

    def own(source, sign, node):
        window = (here + toward * sign * node + replicas) % replicas
        return lax.dynamic_slice(source, (0, window * width), (rows, width))

    def pairs(sign, hops):
        out = []
        for shard in range(shards):
            way = sign if shard % 2 == 0 else -sign
            for z in range(replicas):
                out.append((shard * replicas + z, shard * replicas + (z + way * hops) % replicas))
        return out

    def send(arm, nodes, payload):
        parent, sign, got = arm
        landed = lax.ppermute(payload, ("shard", "rep"), pairs(sign, nodes[0] - parent[nodes[0]]))
        for place, node in enumerate(nodes):
            got[parent[node]].append(landed if len(nodes) == 1 else landed[place])

    def level(parent, step):
        return sorted((n for n in parent if steps_before(parent, n) == step), reverse=True)

    firsts, leaves = [], []
    for arm in arms:
        nodes = level(arm[0], 0)
        chain = [n for n in nodes if arm[0][n] == arm[0][nodes[0]]]
        firsts += [(arm, n) for n in chain]
        leaves.append((arm, [n for n in nodes if n not in chain]))
    slices = [own(partial, arm[1], node) for arm, node in firsts]
    partial, *slices = lax.optimization_barrier((partial, *slices))
    for (arm, node), payload in zip(firsts, slices):
        send(arm, [node], payload)
    last = max(steps_before(parent, node) for parent, _, _ in arms for node in parent)
    held = {(0, 0, 0): own(partial, 1, 0)}
    for index, (parent, sign, _) in enumerate(arms):
        for node in parent:
            if (arms[index], node) not in firsts:
                held[index, node, 0] = own(partial, sign, node)
    held = dict(zip(held, lax.optimization_barrier(tuple(held.values()))))
    for step in range(last + 1):
        todo = []
        for index, arm in enumerate(arms):
            for node in level(arm[0], step) if step else []:
                message = held[index, node, 0]
                for term in arm[2][node]:
                    message = message + term
                todo.append((arm, node, message))
        for index, (arm, nodes) in enumerate(leaves):
            for node in nodes:
                needed = steps_before(arm[0], arm[0][node]) if arm[0][node] else last + 1
                if needed - 2 == step:
                    todo.append((arm, node, held[index, node, 0]))
        if todo:
            payloads = lax.optimization_barrier(tuple(entry[2] for entry in todo))
            for (arm, node, _), payload in zip(todo, payloads):
                send(arm, [node], payload)
    terms = {(0, 0): held[0, 0, 0]}
    return [terms[0, 0]] + [term for _, _, got in arms for term in got[0]]


def dispatch_kernel(terms, owner_ref, *refs):
    term_refs, out_ref = refs[:terms], refs[terms]
    blocks = owner_ref.shape[0]
    width = out_ref.shape[2]
    out_ref[...] = jnp.zeros_like(out_ref)
    for block in range(blocks):
        columns = slice(block * width, (block + 1) * width)
        total = term_refs[0][:, columns].astype(jnp.float32)
        for ref in term_refs[1:]:
            total = total + ref[:, columns].astype(jnp.float32)
        out_ref[owner_ref[block]] = total.astype(jnp.bfloat16)


def mul(first, second):
    return jnp.dot(
        first.astype(jnp.bfloat16), second.astype(jnp.bfloat16), preferred_element_type=jnp.float32
    )


def total_of(values):
    return jnp.sum(jnp.sum(values, axis=0, keepdims=True), axis=1, keepdims=True)


def owner_kernel(me_ref, owner_ref, refresh_ref, grad_ref, roots_ref, out_ref, stat_ref, root_ref):
    size = grad_ref.shape[0]
    me = me_ref[0]
    local_id = jnp.int32(-1)
    for block in range(owner_ref.shape[0]):
        local_id = jnp.where(owner_ref[block] == me, jnp.int32(block), local_id)
    side = jnp.int32(-1)
    for entry in range(refresh_ref.shape[0]):
        value = refresh_ref[entry]
        side = jnp.where(value == 2 * local_id, jnp.int32(0), side)
        side = jnp.where(value == 2 * local_id + 1, jnp.int32(1), side)

    @pl.when(local_id >= 0)
    def _():
        grad = grad_ref[...]
        values = grad.astype(jnp.float32)
        grad_squares = total_of(values * values)

        @pl.when(side != 0)
        def _():
            root_ref[0] = roots_ref[0]

        @pl.when(side != 1)
        def _():
            root_ref[1] = roots_ref[1]

        @pl.when(side == 0)
        def _():
            stat_ref[...] = lax.dot_general(
                grad, grad, (((1,), (1,)), ((), ())), preferred_element_type=jnp.float32
            )

        @pl.when(side == 1)
        def _():
            stat_ref[...] = lax.dot_general(
                grad, grad, (((0,), (0,)), ((), ())), preferred_element_type=jnp.float32
            )

        @pl.when(side >= 0)
        def _():
            rows = lax.broadcasted_iota(jnp.int32, (size, size), 0)
            cols = lax.broadcasted_iota(jnp.int32, (size, size), 1)
            eye = jnp.where(rows == cols, 1.0, 0.0).astype(jnp.float32)
            damped = stat_ref[...] + (damping * grad_squares / size + 1e-06) * eye
            scale = 2.5 / jnp.sqrt(total_of(damped * damped))
            one = damped * scale
            one_low = one.astype(jnp.bfloat16)
            two = mul(one_low, one_low)
            three = mul(two, one_low)
            applied = 1.5625 * one - 0.625 * two + 0.0625 * three
            moment = 1.5625 * applied + mul(0.0625 * two - 0.625 * one, applied)
            root = 1.5625 * eye - 0.3125 * (one + moment) + 0.0625 * mul(one_low, moment)
            root = root * jnp.sqrt(jnp.sqrt(scale))
            root_ref[side] = root.astype(jnp.bfloat16)

        left = jnp.dot(root_ref[0], grad, preferred_element_type=jnp.float32).astype(jnp.bfloat16)
        precon = jnp.dot(left, root_ref[1], preferred_element_type=jnp.float32)
        count = float(size * size)
        graft = jnp.sqrt(
            (grad_squares / count + 1e-06) / (total_of(precon * precon) / count + 1e-06)
        )
        out_ref[...] = (precon * graft).astype(jnp.bfloat16)

    @pl.when(local_id < 0)
    def _():
        out_ref[...] = jnp.zeros_like(out_ref)


def placing_kernel(owner_ref, returned_ref, out_ref):
    width = returned_ref.shape[2]
    for block in range(owner_ref.shape[0]):
        out_ref[:, block * width : (block + 1) * width] = returned_ref[owner_ref[block]]


SMEM = pl.BlockSpec(memory_space=pltpu.SMEM)
VMEM = pl.BlockSpec(memory_space=pltpu.VMEM)


def call(kernel, out_shape, in_specs, scratch, megabytes):
    return pl.pallas_call(
        kernel,
        out_shape=jax.ShapeDtypeStruct(out_shape, jnp.bfloat16),
        in_specs=in_specs,
        out_specs=VMEM,
        scratch_shapes=scratch,
        compiler_params=pltpu.CompilerParams(vmem_limit_bytes=megabytes << 20),
    )


def local(shards, replicas, grad_parts, owner_plan, refresh, roots):
    size = roots.shape[-1]
    rows = grad_parts.shape[1]
    owner_row = owner_plan[0]
    blocks = owner_row.shape[0]
    terms = reduce_windows(grad_parts[0], shards, replicas)
    outgoing = call(
        functools.partial(dispatch_kernel, len(terms)),
        (shards, rows, size),
        [SMEM] + [VMEM] * len(terms),
        [],
        8,
    )(owner_row, *terms)
    incoming = lax.all_to_all(outgoing, "shard", split_axis=0, concat_axis=0, tiled=True)
    update = call(
        owner_kernel,
        (size, size),
        [SMEM, SMEM, SMEM, VMEM, VMEM],
        [pltpu.VMEM((size, size), jnp.float32), pltpu.VMEM((2, size, size), jnp.bfloat16)],
        32,
    )(
        lax.axis_index("shard").astype(jnp.int32)[None],
        owner_row,
        refresh[0],
        incoming.reshape(size, size),
        roots[0, 0],
    )
    returned = lax.all_to_all(
        update.reshape(shards, rows, size), "shard", split_axis=0, concat_axis=0, tiled=True
    )
    return call(placing_kernel, (rows, blocks * size), [SMEM, VMEM], [], 8)(owner_row, returned)


def solution(mesh):
    placed = (
        P("rep", "shard", None),
        P("rep", None),
        P("rep", None),
        P("rep", "shard", None, None, None),
    )
    body = functools.partial(local, mesh.shape["shard"], mesh.shape["rep"])
    return jax.shard_map(
        body, mesh=mesh, in_specs=placed, out_specs=P("shard", "rep"), check_vma=False
    )
```

```python
import functools

import jax
import jax.numpy as jnp
from jax import lax
from jax.experimental import pallas as pl
from jax.experimental.pallas import tpu as pltpu
from jax.sharding import PartitionSpec as P


damping = 0.1

NEWTON = (
    25 / 16,
    -5 / 16 - 3125 / 4096,
    3125 / 4096,
    -1250 / 4096,
    250 / 4096,
    -25 / 4096,
    1 / 4096,
)
STRIP = 64

LONG_ARM = {6: 4, 5: 4, 4: 2, 3: 2, 2: 0, 1: 0}
SHORT_ARM = {5: 4, 4: 2, 3: 2, 2: 0, 1: 0}


def steps_before(parent, node):
    children = [c for c in parent if parent[c] == node]
    return 1 + max(steps_before(parent, c) for c in children) if children else 0


def reduce_windows(partial, shards, replicas):
    rows = partial.shape[0]
    width = partial.shape[1] // replicas
    here = lax.axis_index("rep")
    toward = jnp.where(lax.axis_index("shard") % 2 == 0, 1, -1)
    arms = [
        (LONG_ARM, -1, {node: [] for node in range(7)}),
        (SHORT_ARM, 1, {node: [] for node in range(7)}),
    ]

    def own(source, sign, node):
        window = (here + toward * sign * node + replicas) % replicas
        return lax.dynamic_slice(source, (0, window * width), (rows, width))

    def pairs(sign, hops):
        out = []
        for shard in range(shards):
            way = sign if shard % 2 == 0 else -sign
            for z in range(replicas):
                out.append((shard * replicas + z, shard * replicas + (z + way * hops) % replicas))
        return out

    def send(arm, nodes, payload):
        parent, sign, got = arm
        landed = lax.ppermute(payload, ("shard", "rep"), pairs(sign, nodes[0] - parent[nodes[0]]))
        for place, node in enumerate(nodes):
            got[parent[node]].append(landed if len(nodes) == 1 else landed[place])

    def level(parent, step):
        return sorted((n for n in parent if steps_before(parent, n) == step), reverse=True)

    firsts, leaves = [], []
    for arm in arms:
        nodes = level(arm[0], 0)
        chain = [n for n in nodes if arm[0][n] == arm[0][nodes[0]]]
        firsts += [(arm, n) for n in chain]
        leaves.append((arm, [n for n in nodes if n not in chain]))
    slices = [own(partial, arm[1], node) for arm, node in firsts]
    partial, *slices = lax.optimization_barrier((partial, *slices))
    for (arm, node), payload in zip(firsts, slices):
        send(arm, [node], payload)
    last = max(steps_before(parent, node) for parent, _, _ in arms for node in parent)
    held = {(0, 0, 0): own(partial, 1, 0)}
    for index, (parent, sign, _) in enumerate(arms):
        for node in parent:
            if (arms[index], node) not in firsts:
                held[index, node, 0] = own(partial, sign, node)
    held = dict(zip(held, lax.optimization_barrier(tuple(held.values()))))
    for step in range(last + 1):
        todo = []
        for index, arm in enumerate(arms):
            for node in level(arm[0], step) if step else []:
                message = held[index, node, 0]
                for term in arm[2][node]:
                    message = message + term
                todo.append((arm, node, message))
        for index, (arm, nodes) in enumerate(leaves):
            for node in nodes:
                needed = steps_before(arm[0], arm[0][node]) if arm[0][node] else last + 1
                if needed - 2 == step:
                    todo.append((arm, node, held[index, node, 0]))
        if todo:
            payloads = lax.optimization_barrier(tuple(entry[2] for entry in todo))
            for (arm, node, _), payload in zip(todo, payloads):
                send(arm, [node], payload)
    terms = {(0, 0): held[0, 0, 0]}
    return [terms[0, 0]] + [term for _, _, got in arms for term in got[0]]


def dispatch_kernel(terms, owner_ref, *refs):
    term_refs, out_ref = refs[:terms], refs[terms]
    blocks = owner_ref.shape[0]
    width = out_ref.shape[2]
    for block in range(blocks):
        columns = slice(block * width, (block + 1) * width)
        total = term_refs[0][:, columns].astype(jnp.float32)
        for ref in term_refs[1:]:
            total = total + ref[:, columns].astype(jnp.float32)
        out_ref[owner_ref[block]] = total.astype(jnp.bfloat16)


def mul(first, second):
    return jnp.dot(first, second, preferred_element_type=jnp.float32)


def strips(size):
    return [slice(start, start + STRIP) for start in range(0, size, STRIP)]


def sum_of_squares(size, strip_of):
    total = 0.0
    for strip in strips(size):
        values = strip_of(strip)
        total = total + jnp.sum((values * values).reshape(STRIP // 8, 8, size), axis=0)
    return jnp.sum(jnp.sum(total, axis=0, keepdims=True), axis=1, keepdims=True)


def owner_kernel(
    me_ref, owner_ref, refresh_ref, grad_ref, roots_ref, out_ref, one_ref, two_ref, three_ref, low_ref, root_ref
):
    size = grad_ref.shape[0]
    me = me_ref[0]
    local_id = jnp.int32(-1)
    for block in range(owner_ref.shape[0]):
        local_id = jnp.where(owner_ref[block] == me, jnp.int32(block), local_id)
    side = jnp.int32(-1)
    for entry in range(refresh_ref.shape[0]):
        value = refresh_ref[entry]
        side = jnp.where(value == 2 * local_id, jnp.int32(0), side)
        side = jnp.where(value == 2 * local_id + 1, jnp.int32(1), side)

    def diagonal(strip, value):
        rows = lax.broadcasted_iota(jnp.int32, (STRIP, size), 0) + strip.start
        cols = lax.broadcasted_iota(jnp.int32, (STRIP, size), 1)
        return jnp.where(rows == cols, value, 0.0)

    @pl.when(local_id >= 0)
    def _():
        grad_squares = sum_of_squares(size, lambda strip: grad_ref[strip].astype(jnp.float32))

        @pl.when(side != 0)
        def _():
            root_ref[0] = roots_ref[0]

        @pl.when(side != 1)
        def _():
            root_ref[1] = roots_ref[1]

        @pl.when(side == 0)
        def _():
            one_ref[...] = lax.dot_general(
                grad_ref[...],
                grad_ref[...],
                (((1,), (1,)), ((), ())),
                preferred_element_type=jnp.float32,
            )

        @pl.when(side == 1)
        def _():
            one_ref[...] = lax.dot_general(
                grad_ref[...],
                grad_ref[...],
                (((0,), (0,)), ((), ())),
                preferred_element_type=jnp.float32,
            )

        @pl.when(side >= 0)
        def _():
            ridge = damping * grad_squares / size + 1e-06
            norm = sum_of_squares(size, lambda strip: one_ref[strip] + diagonal(strip, ridge))
            scale = 2.5 / jnp.sqrt(norm)
            for strip in strips(size):
                one = (one_ref[strip] + diagonal(strip, ridge)) * scale
                one_ref[strip] = one
                low_ref[0, strip] = one.astype(jnp.bfloat16)
            two_ref[...] = mul(low_ref[0], low_ref[0])
            for strip in strips(size):
                low_ref[1, strip] = two_ref[strip].astype(jnp.bfloat16)
            three_ref[...] = mul(low_ref[1], low_ref[0])
            for strip in strips(size):
                one, two, three = one_ref[strip], two_ref[strip], three_ref[strip]
                high = NEWTON[4] * one + NEWTON[5] * two + NEWTON[6] * three
                low_ref[0, strip] = three.astype(jnp.bfloat16)
                low_ref[1, strip] = high.astype(jnp.bfloat16)
                rest = NEWTON[1] * one + NEWTON[2] * two + NEWTON[3] * three
                one_ref[strip] = rest + diagonal(strip, NEWTON[0])
            two_ref[...] = mul(low_ref[0], low_ref[1])
            fourth = jnp.sqrt(jnp.sqrt(scale))
            for strip in strips(size):
                root_ref[side, strip] = ((two_ref[strip] + one_ref[strip]) * fourth).astype(
                    jnp.bfloat16
                )

        two_ref[...] = mul(root_ref[0], grad_ref[...])
        for strip in strips(size):
            low_ref[0, strip] = two_ref[strip].astype(jnp.bfloat16)
        one_ref[...] = mul(low_ref[0], root_ref[1])
        count = float(size * size)
        precon_squares = sum_of_squares(size, lambda strip: one_ref[strip])
        graft = jnp.sqrt((grad_squares / count + 1e-06) / (precon_squares / count + 1e-06))
        for strip in strips(size):
            out_ref[strip] = (one_ref[strip] * graft).astype(jnp.bfloat16)

    @pl.when(local_id < 0)
    def _():
        out_ref[...] = jnp.zeros_like(out_ref)


def placing_kernel(owner_ref, returned_ref, out_ref):
    width = returned_ref.shape[2]
    for block in range(owner_ref.shape[0]):
        out_ref[:, block * width : (block + 1) * width] = returned_ref[owner_ref[block]]


SMEM = pl.BlockSpec(memory_space=pltpu.SMEM)
VMEM = pl.BlockSpec(memory_space=pltpu.VMEM)


def call(kernel, out_shape, in_specs, scratch, megabytes):
    return pl.pallas_call(
        kernel,
        out_shape=jax.ShapeDtypeStruct(out_shape, jnp.bfloat16),
        in_specs=in_specs,
        out_specs=VMEM,
        scratch_shapes=scratch,
        compiler_params=pltpu.CompilerParams(vmem_limit_bytes=megabytes << 20),
    )


def local(shards, replicas, grad_parts, owner_plan, refresh, roots):
    size = roots.shape[-1]
    rows = grad_parts.shape[1]
    owner_row = owner_plan[0]
    blocks = owner_row.shape[0]
    terms = reduce_windows(grad_parts[0], shards, replicas)
    outgoing = call(
        functools.partial(dispatch_kernel, len(terms)),
        (shards, rows, size),
        [SMEM] + [VMEM] * len(terms),
        [],
        8,
    )(owner_row, *terms)
    incoming = lax.all_to_all(outgoing, "shard", split_axis=0, concat_axis=0, tiled=True)
    update = call(
        owner_kernel,
        (size, size),
        [SMEM, SMEM, SMEM, VMEM, VMEM],
        [pltpu.VMEM((size, size), jnp.float32)] * 3 + [pltpu.VMEM((2, size, size), jnp.bfloat16)] * 2,
        32,
    )(
        lax.axis_index("shard").astype(jnp.int32)[None],
        owner_row,
        refresh[0],
        incoming.reshape(size, size),
        roots[0, 0],
    )
    returned = lax.all_to_all(
        update.reshape(shards, rows, size), "shard", split_axis=0, concat_axis=0, tiled=True
    )
    return call(placing_kernel, (rows, blocks * size), [SMEM, VMEM], [], 8)(owner_row, returned)


def solution(mesh):
    placed = (
        P("rep", "shard", None),
        P("rep", None),
        P("rep", None),
        P("rep", "shard", None, None, None),
    )
    body = functools.partial(local, mesh.shape["shard"], mesh.shape["rep"])
    return jax.shard_map(
        body, mesh=mesh, in_specs=placed, out_specs=P("shard", "rep"), check_vma=False
    )
```
